16 devices in a mesh: dp: 1, tp: 16 (over x, y, z, core).
Axes of the slice: x: 2, y: 2, z: 2, core: 2. Of those that a mesh axis runs over, the one named last changes fastest.
Arguments:
- x: bfloat16 [2048, 8192], P(('dp', 'tp'))
- dy: bfloat16 [2048, 8192], P(('dp', 'tp'))
- gain: bfloat16 [8192], replicated
- wq: bfloat16 [8192, 8192], P(None, 'tp')
- wk: bfloat16 [8192, 8192], P(None, 'tp')
- wv: bfloat16 [8192, 8192], P(None, 'tp')
- wo: bfloat16 [8192, 8192], P('tp')
Outputs:
- output 1: bfloat16 [2048, 8192], P(('dp', 'tp'))
- output 2: float32 [1, 8192], P('dp')
- output 3: bfloat16 [8192, 8192], P('dp', 'tp')
- output 4: bfloat16 [8192, 8192], P('dp', 'tp')
- output 5: bfloat16 [8192, 8192], P('dp', 'tp')
- output 6: bfloat16 [8192, 8192], P(('dp', 'tp'))
All inputs are finite; a program needn't handle non-finite values.
Results may differ from the reference program's by a relative error of at most 0.018.
Values are sent between devices in bfloat16 or wider.
A program may use at most 2 GiB of HBM per device.

```python
import jax
import jax.numpy as jnp
from jax import lax

ROWS = 2048
D = 8192
HEADS = 64
KV_HEADS = 64
HEAD = 128
THETA = 10000


def setup_inputs(seed: int = 0, part: int = 0) -> dict:
    kx, ky, kn, kq, kk, kv, ko = jax.random.split(jax.random.key(seed), 7)

    def weights(key, rows, columns):
        return jax.random.normal(key, (rows, columns), jnp.float32) * rows**-0.5

    drawn = {
        "x": jax.random.normal(jax.random.fold_in(kx, part), (ROWS, D), jnp.float32),
        "dy": jax.random.normal(jax.random.fold_in(ky, part), (ROWS, D), jnp.float32) * ROWS**-0.5,
        "gain": 1 + 0.1 * jax.random.normal(kn, (D,), jnp.float32),
        "wq": 2 * weights(kq, D, HEADS * HEAD),
        "wk": 2 * weights(kk, D, KV_HEADS * HEAD),
        "wv": 4 * weights(kv, D, KV_HEADS * HEAD),
        "wo": weights(ko, HEADS * HEAD, D),
    }
    return {k: v.astype(jnp.bfloat16) for k, v in drawn.items()}


def normed(x, gain):
    wide = x.astype(jnp.float32)
    scale = lax.rsqrt(jnp.mean(wide * wide, -1, keepdims=True) + 1e-6)
    return (wide * scale * gain.astype(jnp.float32)).astype(jnp.bfloat16)


def turned(t, place, theta):
    half = t.shape[-1] // 2
    angle = place.astype(jnp.float32)[:, None] * theta ** (-jnp.arange(half, dtype=jnp.float32) / half)
    cos, sin = jnp.cos(angle)[:, None], jnp.sin(angle)[:, None]
    a, b = t[..., :half].astype(jnp.float32), t[..., half:].astype(jnp.float32)
    return jnp.concatenate([a * cos - b * sin, b * cos + a * sin], -1).astype(jnp.bfloat16)


def matmul(a, w):
    return jnp.dot(a, w, preferred_element_type=jnp.float32).astype(jnp.bfloat16)


def einsum(form, a, b):
    return jnp.einsum(form, a.astype(jnp.float32), b.astype(jnp.float32))


def attention(q, k, v):
    scores = einsum("tgsd,ugd->gstu", q, k) * q.shape[-1] ** -0.5
    token = jnp.arange(q.shape[0])
    scores = jnp.where(token[:, None] >= token, scores, -jnp.inf)
    weights = jax.nn.softmax(scores, -1).astype(jnp.bfloat16)
    return einsum("gstu,ugd->tgsd", weights, v).astype(jnp.bfloat16)


def forward(x, gain, wq, wk, wv, wo):
    rows = x.shape[0]
    a, place = normed(x, gain), jnp.arange(rows)
    k = turned(matmul(a, wk).reshape(rows, -1, HEAD), place, THETA)
    q = turned(matmul(a, wq).reshape(rows, -1, HEAD), place, THETA).reshape(rows, k.shape[1], -1, HEAD)
    v = matmul(a, wv).reshape(rows, -1, HEAD)
    seen = attention(q, k, v).reshape(rows, -1)
    return (x.astype(jnp.float32) + jnp.dot(seen, wo, preferred_element_type=jnp.float32)).astype(jnp.bfloat16)


def reference(x, dy, gain, wq, wk, wv, wo):
    _, back = jax.vjp(forward, x, gain.astype(jnp.float32), wq, wk, wv, wo)
    by_x, by_gain, *by_weights = back(dy)
    return (by_x, by_gain[None], *by_weights)
```

```python
import functools

import jax
import jax.numpy as jnp
from jax import lax
from jax.experimental import pallas as pl
from jax.experimental.pallas import tpu as pltpu
from jax.sharding import PartitionSpec as P

HEAD = 128
THETA = 10000
NEG = -1e30
HIDDEN = 2 * NEG
LOG2E = 1.4426950408889634
MESH = pl.DeviceIdType.MESH
ANY = pl.BlockSpec(memory_space=pl.ANY)
WHOLE = pl.BlockSpec(memory_space=pltpu.VMEM)
F32, BF16 = jnp.float32, jnp.bfloat16


def _dot(a, b, ca, cb):
    return lax.dot_general(a, b, (((ca,), (cb,)), ((), ())), preferred_element_type=F32)


def _turn(t, cos, sin):
    return t * cos + pltpu.roll(t, HEAD // 2, 1) * sin


def _head(i):
    return slice(i * HEAD, (i + 1) * HEAD)


def _gap(bk, bq):
    return lax.broadcasted_iota(jnp.int32, (bk, bq), 1) - lax.broadcasted_iota(jnp.int32, (bk, bq), 0)


def _attend(q_ref, k_ref, v_ref, cos_ref, sin_ref, o_ref, lse_ref, qr_ref, kr_ref, k_s, top_s, mix_s, *, scale, bq, bk, wide):
    heads = q_ref.shape[1] // HEAD
    iq = pl.program_id(0)
    e = scale * LOG2E
    cos, sin = cos_ref[...], sin_ref[...]
    mine = pl.ds(iq * bq, bq)
    for i in range(heads):
        qr_ref[:, _head(i)] = _turn(q_ref[:, _head(i)].astype(F32), cos, sin).astype(BF16)
        turned = _turn(k_ref[:, _head(i)].astype(F32), cos, sin).astype(BF16)
        kr_ref[:, _head(i)] = turned
        k_s[mine, _head(i)] = turned
        top_s[i : i + 1, :] = jnp.full((1, bq), NEG, F32)
        mix_s[i] = jnp.zeros((HEAD + 8, bq), F32)
    ones = jnp.ones((8, bk), BF16)
    pieces = [(i, at) for i in range(heads) for at in range(0, bq, wide)]

    def block(j, masked):
        here = pl.ds(pl.multiple_of(j * bk, bk), bk)
        scores = [_dot(k_s[here, _head(i)], qr_ref[at : at + wide, _head(i)], 1, 1) for i, at in pieces]
        ok = _gap(bk, bq) >= j * bk - iq * bq if masked else None
        weights, keeps = [], []
        for (i, at), s in zip(pieces, scores):
            if masked:
                s = jnp.where(ok[:, at : at + wide], s, HIDDEN)
            old = top_s[i : i + 1, at : at + wide]
            top = jnp.maximum(old, s.max(axis=0, keepdims=True))
            top_s[i : i + 1, at : at + wide] = top
            weights.append(jnp.exp2((s - top) * e).astype(BF16))
            keeps.append(jnp.exp2((old - top) * e))
        for (i, at), p, keep in zip(pieces, weights, keeps):
            values = jnp.concatenate([v_ref[here, _head(i)].T, ones], axis=0)
            mix_s[i, :, at : at + wide] = mix_s[i, :, at : at + wide] * keep + _dot(values, p, 1, 0)

    whole = iq * (bq // bk)
    lax.fori_loop(0, whole, lambda j, _: block(j, False), None)
    lax.fori_loop(whole, whole + bq // bk, lambda j, _: block(j, True), None)
    for i in range(heads):
        total = mix_s[i, HEAD : HEAD + 1, :]
        o_ref[:, _head(i)] = (mix_s[i, :HEAD, :] * (1 / total)).T.astype(BF16)
        lse_ref[i : i + 1, :] = top_s[i : i + 1, :] * scale + jnp.log(total)


def attend(q, k, v, cos, sin):
    rows, width = q.shape
    heads, bq, bk, wide = width // HEAD, 1024, 512, 512
    block = pl.BlockSpec((bq, width), lambda i: (i, 0))
    table = pl.BlockSpec((bq, HEAD), lambda i: (i, 0))
    like = jax.ShapeDtypeStruct((rows, width), BF16)
    return pl.pallas_call(
        functools.partial(_attend, scale=HEAD**-0.5, bq=bq, bk=bk, wide=wide),
        grid=(rows // bq,),
        in_specs=[block, block, pl.BlockSpec((rows, width), lambda i: (0, 0)), table, table],
        out_specs=[block, pl.BlockSpec((heads, bq), lambda i: (0, i)), block, block],
        out_shape=[like, jax.ShapeDtypeStruct((heads, rows), F32), like, like],
        scratch_shapes=[pltpu.VMEM((rows, width), BF16), pltpu.VMEM((heads, bq), F32), pltpu.VMEM((heads, HEAD + 8, bq), F32)],
        compiler_params=pltpu.CompilerParams(dimension_semantics=("arbitrary",), vmem_limit_bytes=56 * 2**20),
        cost_estimate=pl.CostEstimate(flops=4 * rows * rows * width, transcendentals=heads * rows * rows, bytes_accessed=14 * rows * width),
    )(q, k, v, cos, sin)


def _attend_bwd(q_ref, k_ref, v_ref, do_ref, o_ref, lse_ref, cos_ref, sin_ref, dq_ref, dk_ref, dv_ref, dq_s, dk_s, dv_s, *, scale, bq, bk):
    heads = q_ref.shape[1] // HEAD
    rows = k_ref.shape[0]
    iq = pl.program_id(0)
    e = scale * LOG2E

    @pl.when(iq == 0)
    def _():
        dk_s[...] = jnp.zeros_like(dk_s)
        dv_s[...] = jnp.zeros_like(dv_s)

    dq_s[...] = jnp.zeros_like(dq_s)
    lses = [lse_ref[i : i + 1, :] * LOG2E for i in range(heads)]
    deltas = []
    for i in range(heads):
        both = do_ref[:, _head(i)].astype(F32) * o_ref[:, _head(i)].astype(F32)
        deltas.append(both.T.sum(axis=0, keepdims=True))

    def block(j, masked):
        here = pl.ds(pl.multiple_of(j * bk, bk), bk)
        qs = [q_ref[:, _head(i)] for i in range(heads)]
        dos = [do_ref[:, _head(i)] for i in range(heads)]
        scores = [_dot(k_ref[here, _head(i)], qs[i], 1, 1) for i in range(heads)]
        dps = [_dot(v_ref[here, _head(i)], dos[i], 1, 1) for i in range(heads)]
        ok = _gap(bk, bq) >= j * bk - iq * bq if masked else None
        for i in range(heads):
            p = jnp.exp2(scores[i] * e - lses[i])
            if masked:
                p = jnp.where(ok, p, 0.0)
            ds = (p * (dps[i] - deltas[i])).astype(BF16)
            dv_s[here, _head(i)] += _dot(p.astype(BF16), dos[i], 1, 0)
            dk_s[here, _head(i)] += _dot(ds, qs[i], 1, 0)
            dq_s[i] += _dot(k_ref[here, _head(i)].T, ds, 1, 0)

    whole = iq * (bq // bk)
    lax.fori_loop(0, whole, lambda j, _: block(j, False), None)
    lax.fori_loop(whole, whole + bq // bk, lambda j, _: block(j, True), None)
    mine = pl.ds(pl.multiple_of(iq * bq, bq), bq)
    for i in range(heads):
        dq_ref[:, _head(i)] = _turn((dq_s[i] * scale).T, cos_ref[mine, :], -sin_ref[mine, :]).astype(BF16)

    @pl.when(iq == pl.num_programs(0) - 1)
    def _():
        for r in range(0, rows, 512):
            some = slice(r, r + 512)
            for i in range(heads):
                dk_ref[some, _head(i)] = _turn(dk_s[some, _head(i)] * scale, cos_ref[some, :], -sin_ref[some, :]).astype(BF16)
                dv_ref[some, _head(i)] = dv_s[some, _head(i)].astype(BF16)


def attend_bwd(q, k, v, d_out, out, lse, cos, sin):
    rows, width = q.shape
    heads, bq, bk = width // HEAD, 512, 512
    block = pl.BlockSpec((bq, width), lambda i: (i, 0))
    whole = pl.BlockSpec((rows, width), lambda i: (0, 0))
    table = pl.BlockSpec((rows, HEAD), lambda i: (0, 0))
    like = jax.ShapeDtypeStruct((rows, width), BF16)
    return pl.pallas_call(
        functools.partial(_attend_bwd, scale=HEAD**-0.5, bq=bq, bk=bk),
        grid=(rows // bq,),
        in_specs=[block, whole, whole, block, block, pl.BlockSpec((heads, bq), lambda i: (0, i)), table, table],
        out_specs=[block, whole, whole],
        out_shape=[like, like, like],
        scratch_shapes=[pltpu.VMEM((heads, HEAD, bq), F32), pltpu.VMEM((rows, width), F32), pltpu.VMEM((rows, width), F32)],
        compiler_params=pltpu.CompilerParams(dimension_semantics=("arbitrary",), vmem_limit_bytes=60 * 2**20),
        cost_estimate=pl.CostEstimate(flops=10 * rows * rows * width, transcendentals=heads * rows * rows, bytes_accessed=18 * rows * width),
    )(q, k, v, d_out, out, lse, cos, sin)


CW = 256
L1, L2, L3, L4 = 1, 3, 5, 7
SLOTS = 9
SEND = 4


def _stage_axis(s, c):
    d = lax.rem(c + s - 1, 3)
    return 4 - 2 * d + d // 2


def _tail(dq_ref, dk_ref, dv_ref, wq_ref, wk_ref, wv_ref, x_ref, sum_ref, gq_ref, gk_ref, gv_ref,
          d_s, w_s, x_s, g_s, acc_s, out0, in0, out1, in1, out2, in2, out3, in3,
          d_sem, w_sem, x_sem, g_sem, out_sem, in_sem):
    rows, width = dq_ref.shape
    chunks = wq_ref.shape[0] // CW
    me = lax.axis_index("tp")
    core, chip = lax.rem(me, 2), lax.div(me, 2)
    outs, ins = (out0, out1, out2, out3), (in0, in1, in2, in3)

    def bit(stride):
        return lax.rem(lax.div(chip, stride), 2)

    def partner(s, c):
        if s == 0:
            return me + 1 - 2 * core
        stride = _stage_axis(s, c)
        return me + (1 - 2 * bit(stride)) * stride * 2

    def send(s, c):
        at, to = lax.rem(c, SEND), lax.rem(c, SLOTS)
        return pltpu.make_async_remote_copy(
            src_ref=outs[s].at[at], dst_ref=ins[s].at[to], send_sem=out_sem.at[s, at], recv_sem=in_sem.at[s, to],
            device_id={"tp": partner(s, c)}, device_id_type=MESH)

    def fetch_w(c):
        at = lax.rem(c, 2)
        here = pl.ds(pl.multiple_of(c * CW, CW), CW)
        return [pltpu.make_async_copy(w.at[here, :], w_s.at[at, :, n * width : (n + 1) * width], w_sem.at[at, n])
                for n, w in enumerate((wq_ref, wk_ref, wv_ref))]

    def fetch_x(c):
        at = lax.rem(c, 2)
        return pltpu.make_async_copy(x_ref.at[:, pl.ds(pl.multiple_of(c * CW, CW), CW)], x_s.at[at], x_sem.at[at])

    def store_g(c):
        at = lax.rem(c, 2)
        here = pl.ds(pl.multiple_of(c * CW, CW), CW)
        return [pltpu.make_async_copy(g_s.at[at, :, n * width : (n + 1) * width], g.at[here, :], g_sem.at[at, n])
                for n, g in enumerate((gq_ref, gk_ref, gv_ref))]

    load = [pltpu.make_async_copy(d, d_s.at[:, n * width : (n + 1) * width], d_sem.at[n]) for n, d in enumerate((dq_ref, dk_ref, dv_ref))]
    for copy in load:
        copy.start()
    for copy in fetch_w(0):
        copy.start()
    fetch_x(0).start()
    barrier = pltpu.get_barrier_semaphore()
    others = [me + 1 - 2 * core] + [me + (1 - 2 * bit(stride)) * stride * 2 for stride in (4, 2, 1)]
    for other in others:
        pl.semaphore_signal(barrier, inc=1, device_id={"tp": other}, device_id_type=MESH)
    pl.semaphore_wait(barrier, 4)
    for copy in load:
        copy.wait()

    def step(t, _):
        def stage(s, lag):
            c = t - lag

            @pl.when((c >= 0) & (c < chunks))
            def _():
                s1, s2, s3 = (_stage_axis(n, c) for n in (1, 2, 3))
                b1, b2, b3 = bit(s1), bit(s2), bit(s3)
                acc, slot = lax.rem(c, L4 + 1), lax.rem(c, SLOTS)
                send(s - 1, c).wait_recv()
                if s < 4:
                    @pl.when(c >= SEND)
                    def _():
                        send(s, c - SEND).wait_send()
                n = {1: 4, 2: 2, 3: 1, 4: 1}[s]
                for j in range(n):
                    p2, p3 = {1: (j // 2, j % 2), 2: (1 - b2, j), 3: (b2, 1 - b3), 4: (b2, b3)}[s]
                    block = (1 - b1 if s == 1 else b1) * s1 + p2 * s2 + p3 * s3
                    total = acc_s[acc, block] + in0[slot, block].astype(F32)
                    if s > 1:
                        total += in1[slot, p2 * 2 + p3].astype(F32)
                    if s > 2:
                        total += in2[slot, p3].astype(F32)
                    if s == 4:
                        total += in3[slot, 0].astype(F32)
                        sum_ref[:, pl.ds(pl.multiple_of(c * CW, CW), CW)] = total
                    else:
                        outs[s][lax.rem(c, SEND), j] = total.astype(BF16)
                if s < 4:
                    send(s, c).start()

        stage(4, L4)
        stage(3, L3)
        stage(2, L2)
        stage(1, L1)

        @pl.when(t < chunks)
        def _():
            at = lax.rem(t, 2)
            for copy in fetch_w(t):
                copy.wait()

            @pl.when(t + 1 < chunks)
            def _():
                for copy in fetch_w(t + 1):
                    copy.start()

            @pl.when(t >= SEND)
            def _():
                send(0, t - SEND).wait_send()

            d = d_s.reshape(rows // 256, 2, 128, 3 * width)
            theirs = _dot(d[:, 1 - core].reshape(rows // 2, 3 * width), w_s[at], 1, 1)
            out0[lax.rem(t, SEND)] = theirs.astype(BF16).reshape(rows // 256, 128, CW)
            send(0, t).start()
            ours = _dot(d[:, core].reshape(rows // 2, 3 * width), w_s[at], 1, 1)
            acc_s[lax.rem(t, L4 + 1)] = ours.reshape(rows // 256, 128, CW)

        c = t - L4

        @pl.when(c >= 0)
        def _():
            at = lax.rem(c, 2)
            fetch_x(c).wait()

            @pl.when(c + 1 < chunks)
            def _():
                fetch_x(c + 1).start()

            @pl.when(c >= 2)
            def _():
                for copy in store_g(c - 2):
                    copy.wait()

            g_s[at] = _dot(x_s[at], d_s[...], 0, 0).astype(BF16)
            for copy in store_g(c):
                copy.start()

    lax.fori_loop(0, chunks + L4, step, None)
    for c in (chunks - 2, chunks - 1):
        for copy in store_g(c):
            copy.wait()
    for c in range(chunks - SEND, chunks):
        for s in range(4):
            send(s, c).wait_send()


def tail(dq, dk, dv, wq, wk, wv, x):
    rows, width = dq.shape
    cols = wq.shape[0]
    blocks = rows // 256

    def slots(n, b):
        return pltpu.VMEM((n, b, 128, CW), BF16)

    like = jax.ShapeDtypeStruct((cols, width), BF16)
    return pl.pallas_call(
        _tail,
        in_specs=[ANY] * 7,
        out_specs=[WHOLE, ANY, ANY, ANY],
        out_shape=[jax.ShapeDtypeStruct((128, cols), F32), like, like, like],
        scratch_shapes=[
            pltpu.VMEM((rows, 3 * width), BF16), pltpu.VMEM((2, CW, 3 * width), BF16), pltpu.VMEM((2, rows, CW), BF16),
            pltpu.VMEM((2, CW, 3 * width), BF16), pltpu.VMEM((L4 + 1, blocks, 128, CW), F32),
            slots(SEND, blocks), slots(SLOTS, blocks), slots(SEND, blocks // 2), slots(SLOTS, blocks // 2),
            slots(SEND, blocks // 4), slots(SLOTS, blocks // 4), slots(SEND, blocks // 8), slots(SLOTS, blocks // 8),
            pltpu.SemaphoreType.DMA((3,)), pltpu.SemaphoreType.DMA((2, 3)), pltpu.SemaphoreType.DMA((2,)), pltpu.SemaphoreType.DMA((2, 3)),
            pltpu.SemaphoreType.DMA((4, SEND)), pltpu.SemaphoreType.DMA((4, SLOTS)),
        ],
        compiler_params=pltpu.CompilerParams(collective_id=1, has_side_effects=True, vmem_limit_bytes=62 * 2**20),
        cost_estimate=pl.CostEstimate(flops=12 * rows * width * cols, transcendentals=0, bytes_accessed=16 * cols * width),
    )(dq, dk, dv, wq, wk, wv, x)


def matmul(a, w):
    return jnp.dot(a, w, preferred_element_type=F32).astype(BF16)


def solution(mesh):
    def step(x, dy, gain, wq, wk, wv, wo):
        wide, gain = x.astype(F32), gain.astype(F32)
        scale = lax.rsqrt(jnp.mean(wide * wide, -1, keepdims=True) + 1e-6)
        some = lax.all_gather((wide * scale * gain).astype(BF16), "tp", axis=0, tiled=True)
        dys = lax.all_gather(dy, "tp", axis=0, tiled=True)
        rows = some.shape[0]
        half = HEAD // 2
        angle = jnp.arange(rows).astype(F32)[:, None] * THETA ** (-jnp.arange(half, dtype=F32) / half)
        cos, sin = jnp.cos(angle), jnp.sin(angle)
        cos, sin = jnp.concatenate([cos, cos], 1), jnp.concatenate([-sin, sin], 1)

        v = matmul(some, wv)
        out, lse, q, k = attend(matmul(some, wq), matmul(some, wk), v, cos, sin)
        d_out = lax.dot_general(dys, wo, (((1,), (1,)), ((), ())), preferred_element_type=F32).astype(BF16)
        dq, dk, dv = attend_bwd(q, k, v, d_out, out, lse, cos, sin)
        by_wo = lax.dot_general(out, dys, (((0,), (0,)), ((), ())), preferred_element_type=F32).astype(BF16)
        da, by_wq, by_wk, by_wv = tail(dq, dk, dv, wq, wk, wv, some)

        n = wide * scale
        by_gain = lax.all_gather((da * n).sum(0, keepdims=True), "tp", axis=0, tiled=True).sum(0, keepdims=True)
        dn = da * gain
        by_x = scale * (dn - n * jnp.mean(dn * n, -1, keepdims=True)) + dy.astype(F32)
        return by_x.astype(BF16), by_gain, by_wq, by_wk, by_wv, by_wo

    tokens, columns = P(("dp", "tp"), None), P(None, "tp")
    return jax.shard_map(
        step,
        mesh=mesh,
        in_specs=(tokens, tokens, P(None), columns, columns, columns, P("tp", None)),
        out_specs=(tokens, P("dp", None), P("dp", "tp"), P("dp", "tp"), P("dp", "tp"), P(("dp", "tp"), None)),
        check_vma=False,
    )
```

```python
import functools

import jax
import jax.numpy as jnp
from jax import lax
from jax.experimental import pallas as pl
from jax.experimental.pallas import tpu as pltpu
from jax.sharding import PartitionSpec as P

HEAD = 128
THETA = 10000
NEG = -1e30
HIDDEN = 2 * NEG
LOG2E = 1.4426950408889634
MESH = pl.DeviceIdType.MESH
ANY = pl.BlockSpec(memory_space=pl.ANY)
WHOLE = pl.BlockSpec(memory_space=pltpu.VMEM)
F32, BF16 = jnp.float32, jnp.bfloat16


def _dot(a, b, ca, cb):
    return lax.dot_general(a, b, (((ca,), (cb,)), ((), ())), preferred_element_type=F32)


def _turn(t, cos, sin):
    return t * cos + pltpu.roll(t, HEAD // 2, 1) * sin


def _head(i):
    return slice(i * HEAD, (i + 1) * HEAD)


def _gap(bk, bq):
    return lax.broadcasted_iota(jnp.int32, (bk, bq), 1) - lax.broadcasted_iota(jnp.int32, (bk, bq), 0)


def _attend(q_ref, k_ref, v_ref, cos_ref, sin_ref, o_ref, lse_ref, qr_ref, kr_ref, k_s, top_s, mix_s, *, scale, bq, bk, wide):
    heads = q_ref.shape[1] // HEAD
    iq = pl.program_id(0)
    e = scale * LOG2E
    cos, sin = cos_ref[...], sin_ref[...]
    mine = pl.ds(iq * bq, bq)
    for i in range(heads):
        qr_ref[:, _head(i)] = _turn(q_ref[:, _head(i)].astype(F32), cos, sin).astype(BF16)
        turned = _turn(k_ref[:, _head(i)].astype(F32), cos, sin).astype(BF16)
        kr_ref[:, _head(i)] = turned
        k_s[mine, _head(i)] = turned
        top_s[i : i + 1, :] = jnp.full((1, bq), NEG, F32)
        mix_s[i] = jnp.zeros((HEAD + 8, bq), F32)
    ones = jnp.ones((8, bk), BF16)
    pieces = [(i, at) for i in range(heads) for at in range(0, bq, wide)]

    def block(j, masked):
        here = pl.ds(pl.multiple_of(j * bk, bk), bk)
        scores = [_dot(k_s[here, _head(i)], qr_ref[at : at + wide, _head(i)], 1, 1) for i, at in pieces]
        ok = _gap(bk, bq) >= j * bk - iq * bq if masked else None
        weights, keeps = [], []
        for (i, at), s in zip(pieces, scores):
            if masked:
                s = jnp.where(ok[:, at : at + wide], s, HIDDEN)
            old = top_s[i : i + 1, at : at + wide]
            top = jnp.maximum(old, s.max(axis=0, keepdims=True))
            top_s[i : i + 1, at : at + wide] = top
            weights.append(jnp.exp2((s - top) * e).astype(BF16))
            keeps.append(jnp.exp2((old - top) * e))
        for (i, at), p, keep in zip(pieces, weights, keeps):
            values = jnp.concatenate([v_ref[here, _head(i)].T, ones], axis=0)
            mix_s[i, :, at : at + wide] = mix_s[i, :, at : at + wide] * keep + _dot(values, p, 1, 0)

    whole = iq * (bq // bk)
    lax.fori_loop(0, whole, lambda j, _: block(j, False), None)
    lax.fori_loop(whole, whole + bq // bk, lambda j, _: block(j, True), None)
    for i in range(heads):
        total = mix_s[i, HEAD : HEAD + 1, :]
        o_ref[:, _head(i)] = (mix_s[i, :HEAD, :] * (1 / total)).T.astype(BF16)
        lse_ref[i : i + 1, :] = top_s[i : i + 1, :] * scale + jnp.log(total)


def attend(q, k, v, cos, sin):
    rows, width = q.shape
    heads, bq, bk, wide = width // HEAD, 1024, 512, 512
    block = pl.BlockSpec((bq, width), lambda i: (i, 0))
    table = pl.BlockSpec((bq, HEAD), lambda i: (i, 0))
    like = jax.ShapeDtypeStruct((rows, width), BF16)
    return pl.pallas_call(
        functools.partial(_attend, scale=HEAD**-0.5, bq=bq, bk=bk, wide=wide),
        grid=(rows // bq,),
        in_specs=[block, block, pl.BlockSpec((rows, width), lambda i: (0, 0)), table, table],
        out_specs=[block, pl.BlockSpec((heads, bq), lambda i: (0, i)), block, block],
        out_shape=[like, jax.ShapeDtypeStruct((heads, rows), F32), like, like],
        scratch_shapes=[pltpu.VMEM((rows, width), BF16), pltpu.VMEM((heads, bq), F32), pltpu.VMEM((heads, HEAD + 8, bq), F32)],
        compiler_params=pltpu.CompilerParams(dimension_semantics=("arbitrary",), vmem_limit_bytes=56 * 2**20),
        cost_estimate=pl.CostEstimate(flops=4 * rows * rows * width, transcendentals=heads * rows * rows, bytes_accessed=14 * rows * width),
    )(q, k, v, cos, sin)


def _attend_bwd(q_ref, k_ref, v_ref, do_ref, o_ref, lse_ref, cos_ref, sin_ref, dq_ref, dk_ref, dv_ref, dq_s, dk_s, dv_s, *, scale, bq, bk):
    heads = q_ref.shape[1] // HEAD
    rows = k_ref.shape[0]
    iq = pl.program_id(0)
    e = scale * LOG2E

    @pl.when(iq == 0)
    def _():
        dk_s[...] = jnp.zeros_like(dk_s)
        dv_s[...] = jnp.zeros_like(dv_s)

    dq_s[...] = jnp.zeros_like(dq_s)
    lses = [lse_ref[i : i + 1, :] * LOG2E for i in range(heads)]
    deltas = []
    for i in range(heads):
        both = do_ref[:, _head(i)].astype(F32) * o_ref[:, _head(i)].astype(F32)
        deltas.append(both.T.sum(axis=0, keepdims=True))

    def block(j, masked):
        here = pl.ds(pl.multiple_of(j * bk, bk), bk)
        qs = [q_ref[:, _head(i)] for i in range(heads)]
        dos = [do_ref[:, _head(i)] for i in range(heads)]
        scores = [_dot(k_ref[here, _head(i)], qs[i], 1, 1) for i in range(heads)]
        dps = [_dot(v_ref[here, _head(i)], dos[i], 1, 1) for i in range(heads)]
        ok = _gap(bk, bq) >= j * bk - iq * bq if masked else None
        for i in range(heads):
            p = jnp.exp2(scores[i] * e - lses[i])
            if masked:
                p = jnp.where(ok, p, 0.0)
            ds = (p * (dps[i] - deltas[i])).astype(BF16)
            dv_s[here, _head(i)] += _dot(p.astype(BF16), dos[i], 1, 0)
            dk_s[here, _head(i)] += _dot(ds, qs[i], 1, 0)
            dq_s[i] += _dot(k_ref[here, _head(i)].T, ds, 1, 0)

    whole = iq * (bq // bk)
    lax.fori_loop(0, whole, lambda j, _: block(j, False), None)
    lax.fori_loop(whole, whole + bq // bk, lambda j, _: block(j, True), None)
    mine = pl.ds(pl.multiple_of(iq * bq, bq), bq)
    for i in range(heads):
        dq_ref[:, _head(i)] = _turn((dq_s[i] * scale).T, cos_ref[mine, :], -sin_ref[mine, :]).astype(BF16)

    @pl.when(iq == pl.num_programs(0) - 1)
    def _():
        for r in range(0, rows, 512):
            some = slice(r, r + 512)
            for i in range(heads):
                dk_ref[some, _head(i)] = _turn(dk_s[some, _head(i)] * scale, cos_ref[some, :], -sin_ref[some, :]).astype(BF16)
                dv_ref[some, _head(i)] = dv_s[some, _head(i)].astype(BF16)


def attend_bwd(q, k, v, d_out, out, lse, cos, sin):
    rows, width = q.shape
    heads, bq, bk = width // HEAD, 512, 512
    block = pl.BlockSpec((bq, width), lambda i: (i, 0))
    whole = pl.BlockSpec((rows, width), lambda i: (0, 0))
    table = pl.BlockSpec((rows, HEAD), lambda i: (0, 0))
    like = jax.ShapeDtypeStruct((rows, width), BF16)
    return pl.pallas_call(
        functools.partial(_attend_bwd, scale=HEAD**-0.5, bq=bq, bk=bk),
        grid=(rows // bq,),
        in_specs=[block, whole, whole, block, block, pl.BlockSpec((heads, bq), lambda i: (0, i)), table, table],
        out_specs=[block, whole, whole],
        out_shape=[like, like, like],
        scratch_shapes=[pltpu.VMEM((heads, HEAD, bq), F32), pltpu.VMEM((rows, width), F32), pltpu.VMEM((rows, width), F32)],
        compiler_params=pltpu.CompilerParams(dimension_semantics=("arbitrary",), vmem_limit_bytes=60 * 2**20),
        cost_estimate=pl.CostEstimate(flops=10 * rows * rows * width, transcendentals=heads * rows * rows, bytes_accessed=18 * rows * width),
    )(q, k, v, d_out, out, lse, cos, sin)


CW = 256
L1, L2, L3, L4 = 2, 7, 11, 14
SLOTS = 18
SEND = 4
AHEAD = 2


def _stage_axis(s, c):
    d = lax.rem(c + s - 1, 3)
    return 4 - 2 * d + d // 2


def _tail(dq_ref, dk_ref, dv_ref, wq_ref, wk_ref, wv_ref, x_ref, sum_ref, gq_ref, gk_ref, gv_ref,
          d_s, w_s, x_s, g_s, acc_s, out0, in0, out1, in1, out2, in2, out3, in3,
          d_sem, w_sem, x_sem, g_sem, out_sem, in_sem):
    rows, width = x_ref.shape[0], wq_ref.shape[1]
    chunks = wq_ref.shape[0] // CW
    me = lax.axis_index("tp")
    core, chip = lax.rem(me, 2), lax.div(me, 2)
    outs, ins = (out0, out1, out2, out3), (in0, in1, in2, in3)

    def bit(stride):
        return lax.rem(lax.div(chip, stride), 2)

    def partner(s, c):
        if s == 0:
            return me + 1 - 2 * core
        stride = _stage_axis(s, c)
        return me + (1 - 2 * bit(stride)) * stride * 2

    def send(s, c):
        at, to = lax.rem(c, SEND), lax.rem(c, SLOTS)
        return pltpu.make_async_remote_copy(
            src_ref=outs[s].at[at], dst_ref=ins[s].at[to], send_sem=out_sem.at[s, at], recv_sem=in_sem.at[s, to],
            device_id={"tp": partner(s, c)}, device_id_type=MESH)

    def fetch_w(c):
        at = lax.rem(c, AHEAD)
        here = pl.ds(pl.multiple_of(c * CW, CW), CW)
        return [pltpu.make_async_copy(w.at[here, :], w_s.at[at, :, n * width : (n + 1) * width], w_sem.at[at, n])
                for n, w in enumerate((wq_ref, wk_ref, wv_ref))]

    def fetch_x(c):
        at = lax.rem(c, AHEAD)
        return pltpu.make_async_copy(x_ref.at[:, pl.ds(pl.multiple_of(c * CW, CW), CW)], x_s.at[at], x_sem.at[at])

    def store_g(c):
        at = lax.rem(c, AHEAD)
        here = pl.ds(pl.multiple_of(c * CW, CW), CW)
        return [pltpu.make_async_copy(g_s.at[at, :, n * width : (n + 1) * width], g.at[here, :], g_sem.at[at, n])
                for n, g in enumerate((gq_ref, gk_ref, gv_ref))]

    load = [pltpu.make_async_copy(d, d_s.at[:, :, :, n * width : (n + 1) * width], d_sem.at[n]) for n, d in enumerate((dq_ref, dk_ref, dv_ref))]
    for copy in load:
        copy.start()
    for c in range(AHEAD - 1):
        for copy in fetch_w(c):
            copy.start()
        fetch_x(c).start()
    barrier = pltpu.get_barrier_semaphore()
    others = [me + 1 - 2 * core] + [me + (1 - 2 * bit(stride)) * stride * 2 for stride in (4, 2, 1)]
    for other in others:
        pl.semaphore_signal(barrier, inc=1, device_id={"tp": other}, device_id_type=MESH)
    pl.semaphore_wait(barrier, 4)
    for copy in load:
        copy.wait()

    def step(t, _):
        def stage(s, lag):
            c = t - lag

            @pl.when((c >= 0) & (c < chunks))
            def _():
                s1, s2, s3 = (_stage_axis(n, c) for n in (1, 2, 3))
                b1, b2, b3 = bit(s1), bit(s2), bit(s3)
                acc, slot = lax.rem(c, L4 + 1), lax.rem(c, SLOTS)
                send(s - 1, c).wait_recv()
                if s < 4:
                    @pl.when(c >= SEND)
                    def _():
                        send(s, c - SEND).wait_send()
                n = {1: 4, 2: 2, 3: 1, 4: 1}[s]
                for j in range(n):
                    p2, p3 = {1: (j // 2, j % 2), 2: (1 - b2, j), 3: (b2, 1 - b3), 4: (b2, b3)}[s]
                    block = (1 - b1 if s == 1 else b1) * s1 + p2 * s2 + p3 * s3
                    total = acc_s[acc, block] + in0[slot, block].astype(F32)
                    if s > 1:
                        total += in1[slot, p2 * 2 + p3].astype(F32)
                    if s > 2:
                        total += in2[slot, p3].astype(F32)
                    if s == 4:
                        total += in3[slot, 0].astype(F32)
                        sum_ref[:, pl.ds(pl.multiple_of(c * CW, CW), CW)] = total
                    else:
                        outs[s][lax.rem(c, SEND), j] = total.astype(BF16)
                if s < 4:
                    send(s, c).start()

        stage(4, L4)
        stage(3, L3)
        stage(2, L2)
        stage(1, L1)

        @pl.when(t < chunks)
        def _():
            at = lax.rem(t, AHEAD)
            for copy in fetch_w(t):
                copy.wait()

            @pl.when(t + AHEAD - 1 < chunks)
            def _():
                for copy in fetch_w(t + AHEAD - 1):
                    copy.start()

            @pl.when(t >= SEND)
            def _():
                send(0, t - SEND).wait_send()

            for m in range(0, rows // 256, 2):
                theirs = _dot(d_s[m : m + 2, 1 - core].reshape(256, 3 * width), w_s[at], 1, 1)
                out0[lax.rem(t, SEND), m : m + 2] = theirs.astype(BF16).reshape(2, 128, CW)
            send(0, t).start()
            for m in range(0, rows // 256, 2):
                ours = _dot(d_s[m : m + 2, core].reshape(256, 3 * width), w_s[at], 1, 1)
                acc_s[lax.rem(t, L4 + 1), m : m + 2] = ours.reshape(2, 128, CW)

        c = t - L4

        @pl.when(c >= 0)
        def _():
            at = lax.rem(c, AHEAD)
            fetch_x(c).wait()

            @pl.when(c + AHEAD - 1 < chunks)
            def _():
                fetch_x(c + AHEAD - 1).start()

            @pl.when(c >= AHEAD)
            def _():
                for copy in store_g(c - AHEAD):
                    copy.wait()

            g_s[at] = _dot(x_s[at], d_s[...].reshape(rows, 3 * width), 0, 0).astype(BF16)
            for copy in store_g(c):
                copy.start()

    lax.fori_loop(0, chunks + L4, step, None)
    for c in range(chunks - AHEAD, chunks):
        for copy in store_g(c):
            copy.wait()
    for c in range(chunks - SEND, chunks):
        for s in range(4):
            send(s, c).wait_send()


def tail(dq, dk, dv, wq, wk, wv, x):
    rows, width = dq.shape
    cols = wq.shape[0]
    blocks = rows // 256

    def slots(n, b):
        return pltpu.VMEM((n, b, 128, CW), BF16)

    like = jax.ShapeDtypeStruct((cols, width), BF16)
    return pl.pallas_call(
        _tail,
        in_specs=[ANY] * 7,
        out_specs=[WHOLE, ANY, ANY, ANY],
        out_shape=[jax.ShapeDtypeStruct((128, cols), F32), like, like, like],
        scratch_shapes=[
            pltpu.VMEM((blocks, 2, 128, 3 * width), BF16), pltpu.VMEM((AHEAD, CW, 3 * width), BF16), pltpu.VMEM((AHEAD, rows, CW), BF16),
            pltpu.VMEM((AHEAD, CW, 3 * width), BF16), pltpu.VMEM((L4 + 1, blocks, 128, CW), F32),
            slots(SEND, blocks), slots(SLOTS, blocks), slots(SEND, blocks // 2), slots(SLOTS, blocks // 2),
            slots(SEND, blocks // 4), slots(SLOTS, blocks // 4), slots(SEND, blocks // 8), slots(SLOTS, blocks // 8),
            pltpu.SemaphoreType.DMA((3,)), pltpu.SemaphoreType.DMA((AHEAD, 3)), pltpu.SemaphoreType.DMA((AHEAD,)), pltpu.SemaphoreType.DMA((AHEAD, 3)),
            pltpu.SemaphoreType.DMA((4, SEND)), pltpu.SemaphoreType.DMA((4, SLOTS)),
        ],
        compiler_params=pltpu.CompilerParams(collective_id=1, has_side_effects=True, vmem_limit_bytes=62 * 2**20),
        cost_estimate=pl.CostEstimate(flops=12 * rows * width * cols, transcendentals=0, bytes_accessed=16 * cols * width),
    )(*(d.reshape(blocks, 2, 128, width) for d in (dq, dk, dv)), wq, wk, wv, x)


G2, G3, G4, G5 = 3, 6, 10, 11


class _Gather:
    def __init__(self, mine_ref, buf, local_sem, out_sem, in_sem):
        self.mine_ref, self.buf, self.local_sem, self.out_sem, self.in_sem = mine_ref, buf, local_sem, out_sem, in_sem
        self.chunks = buf.shape[0]
        self.me = lax.axis_index("tp")
        self.core, self.chip = lax.rem(self.me, 2), lax.div(self.me, 2)

    def across(self, chip, stride):
        return chip + (1 - 2 * lax.rem(lax.div(chip, stride), 2)) * stride

    def local(self, c):
        cols = pl.ds(pl.multiple_of(c * CW, CW), CW)
        return pltpu.make_async_copy(self.mine_ref.at[:, cols], self.buf.at[c, self.chip, self.core], self.local_sem.at[c])

    def enter(self):
        lax.fori_loop(0, self.chunks, lambda c, _: self.local(c).start(), None)
        barrier = pltpu.get_barrier_semaphore()
        for other in [2 * self.chip + 1 - self.core] + [2 * self.across(self.chip, stride) + self.core for stride in (4, 2, 1)]:
            pl.semaphore_signal(barrier, inc=1, device_id={"tp": other}, device_id_type=MESH)
        pl.semaphore_wait(barrier, 4)

    def send(self, s, c):
        if s == 4:
            block = self.buf.at[c, :, self.core]
            pltpu.make_async_remote_copy(src_ref=block, dst_ref=block, send_sem=self.out_sem.at[3, c], recv_sem=self.in_sem.at[3, c],
                                         device_id={"tp": 2 * self.chip + 1 - self.core}, device_id_type=MESH).start()
            return
        held = [self.chip]
        for n in range(1, s):
            held += [self.across(chip, _stage_axis(n, c)) for chip in held]
        to = 2 * self.across(self.chip, _stage_axis(s, c)) + self.core
        for chip in held:
            block = self.buf.at[c, chip, self.core]
            pltpu.make_async_remote_copy(src_ref=block, dst_ref=block, send_sem=self.out_sem.at[s - 1, c], recv_sem=self.in_sem.at[s - 1, c],
                                         device_id={"tp": to}, device_id_type=MESH).start()

    def all_of(self, s, c):
        some = self.buf.at[c, pl.ds(0, 2 ** (s - 1)), self.core]
        return pltpu.make_async_remote_copy(src_ref=some, dst_ref=some, send_sem=self.out_sem.at[s - 1, c], recv_sem=self.in_sem.at[s - 1, c],
                                            device_id={"tp": 2 * self.chip + 1 - self.core}, device_id_type=MESH)

    def step(self, t):
        for s, lag, before in ((5, G5, G4), (4, G4, G3), (3, G3, G2), (2, G2, 0)):
            c = t - lag

            @pl.when((c >= 0) & (c < self.chunks))
            def _(s=s, c=c):
                self.all_of(s - 1, c).wait_recv()
                if s < 5:
                    self.send(s, c)

        @pl.when(t < self.chunks)
        def _():
            self.local(t).wait()
            self.send(1, t)

    def leave(self):
        def one(c, _):
            for s in (1, 2, 3, 4):
                self.all_of(s, c).wait_send()

        lax.fori_loop(0, self.chunks, one, None)


def _gather_scratch(chunks):
    return [pltpu.VMEM((chunks, 8, 2, 128, CW), BF16), pltpu.SemaphoreType.DMA((chunks,)),
            pltpu.SemaphoreType.DMA((4, chunks)), pltpu.SemaphoreType.DMA((4, chunks))]


def _project(x_ref, wq_ref, wk_ref, wv_ref, all_ref, q_ref, k_ref, v_ref, buf, local_sem, out_sem, in_sem, w_s, acc_s, r_s, w_sem, all_sem, r_sem):
    width = wq_ref.shape[1]
    chunks = buf.shape[0]
    rows = 16 * 128
    gather = _Gather(x_ref, buf, local_sem, out_sem, in_sem)

    def fetch(c):
        at = lax.rem(c, 2)
        here = pl.ds(pl.multiple_of(c * CW, CW), CW)
        return [pltpu.make_async_copy(w.at[here, :], w_s.at[at, :, n * width : (n + 1) * width], w_sem.at[at, n])
                for n, w in enumerate((wq_ref, wk_ref, wv_ref))]

    def keep(c):
        return pltpu.make_async_copy(buf.at[c], all_ref.at[:, :, :, pl.ds(pl.multiple_of(c * CW, CW), CW)], all_sem.at[c])

    for copy in fetch(0):
        copy.start()
    gather.enter()
    acc_s[...] = jnp.zeros_like(acc_s)

    def step(t, _):
        gather.step(t)
        c = t - G5

        @pl.when(c >= 0)
        def _():
            keep(c).start()
            for copy in fetch(c):
                copy.wait()

            @pl.when(c + 1 < chunks)
            def _():
                for copy in fetch(c + 1):
                    copy.start()

            at = lax.rem(c, 2)
            for n in range(3):
                here = slice(n * width, (n + 1) * width)
                acc_s[:, here] += _dot(buf[c].reshape(rows, CW), w_s[at, :, here], 1, 0)

    lax.fori_loop(0, chunks + G5, step, None)
    results = []
    for n, ref in enumerate((q_ref, k_ref, v_ref)):
        r_s[:, n * width : (n + 1) * width] = acc_s[:, n * width : (n + 1) * width].astype(BF16)
        results.append(pltpu.make_async_copy(r_s.at[:, n * width : (n + 1) * width], ref, r_sem.at[n]))
        results[-1].start()
    gather.leave()
    lax.fori_loop(0, chunks, lambda c, _: keep(c).wait(), None)
    for copy in results:
        copy.wait()


def project(x, wq, wk, wv):
    cols, width = wq.shape
    chunks, rows = cols // CW, 16 * x.shape[0]
    like = jax.ShapeDtypeStruct((rows, width), BF16)
    some, q, k, v = pl.pallas_call(
        _project,
        in_specs=[ANY] * 4,
        out_specs=[ANY] * 4,
        out_shape=[jax.ShapeDtypeStruct((8, 2, 128, cols), BF16), like, like, like],
        scratch_shapes=_gather_scratch(chunks) + [
            pltpu.VMEM((2, CW, 3 * width), BF16), pltpu.VMEM((rows, 3 * width), F32), pltpu.VMEM((rows, 3 * width), BF16),
            pltpu.SemaphoreType.DMA((2, 3)), pltpu.SemaphoreType.DMA((chunks,)), pltpu.SemaphoreType.DMA((3,))],
        compiler_params=pltpu.CompilerParams(collective_id=2, has_side_effects=True, vmem_limit_bytes=63 * 2**20),
        cost_estimate=pl.CostEstimate(flops=6 * rows * width * cols, transcendentals=0, bytes_accessed=8 * cols * width),
    )(x, wq, wk, wv)
    return some.reshape(rows, cols), q, k, v


def _unproject(dy_ref, out_ref, wo_ref, d_ref, gwo_ref, buf, local_sem, out_sem, in_sem, o_s, ot_s, w_s, g_s, acc_s, d_s, o_sem, w_sem, g_sem, d_sem):
    rows, width = out_ref.shape
    chunks = buf.shape[0]
    gather = _Gather(dy_ref, buf, local_sem, out_sem, in_sem)

    def fetch(c):
        at = lax.rem(c, 2)
        return pltpu.make_async_copy(wo_ref.at[:, pl.ds(pl.multiple_of(c * CW, CW), CW)], w_s.at[at], w_sem.at[at])

    def store(c):
        at = lax.rem(c, 2)
        return pltpu.make_async_copy(g_s.at[at], gwo_ref.at[:, pl.ds(pl.multiple_of(c * CW, CW), CW)], g_sem.at[at])

    load = pltpu.make_async_copy(out_ref, o_s, o_sem)
    load.start()
    fetch(0).start()
    gather.enter()
    acc_s[...] = jnp.zeros_like(acc_s)
    load.wait()

    def step(t, _):
        gather.step(t)

        @pl.when(t < 4)
        def _():
            here = pl.ds(pl.multiple_of(t * 512, 512), 512)
            ot_s[:, here] = o_s[here, :].T

        c = t - G5

        @pl.when(c >= 0)
        def _():
            at = lax.rem(c, 2)
            fetch(c).wait()

            @pl.when(c + 1 < chunks)
            def _():
                fetch(c + 1).start()

            @pl.when(c >= 2)
            def _():
                store(c - 2).wait()

            some = buf[c].reshape(rows, CW)
            acc_s[...] += _dot(some, w_s[at], 1, 1)
            g_s[at] = _dot(ot_s[...], some, 1, 0).astype(BF16)
            store(c).start()

    lax.fori_loop(0, chunks + G5, step, None)
    d_s[...] = acc_s[...].astype(BF16)
    result = pltpu.make_async_copy(d_s, d_ref, d_sem)
    result.start()
    gather.leave()
    store(chunks - 2).wait()
    store(chunks - 1).wait()
    result.wait()


def unproject(dy, out, wo):
    rows, width = out.shape
    cols = wo.shape[1]
    chunks = cols // CW
    return pl.pallas_call(
        _unproject,
        in_specs=[ANY] * 3,
        out_specs=[ANY] * 2,
        out_shape=[jax.ShapeDtypeStruct((rows, width), BF16), jax.ShapeDtypeStruct((width, cols), BF16)],
        scratch_shapes=_gather_scratch(chunks) + [
            pltpu.VMEM((rows, width), BF16), pltpu.VMEM((width, rows), BF16), pltpu.VMEM((2, width, CW), BF16), pltpu.VMEM((2, width, CW), BF16),
            pltpu.VMEM((rows, width), F32), pltpu.VMEM((rows, width), BF16),
            pltpu.SemaphoreType.DMA, pltpu.SemaphoreType.DMA((2,)), pltpu.SemaphoreType.DMA((2,)), pltpu.SemaphoreType.DMA],
        compiler_params=pltpu.CompilerParams(collective_id=3, has_side_effects=True, vmem_limit_bytes=63 * 2**20),
        cost_estimate=pl.CostEstimate(flops=4 * rows * width * cols, transcendentals=0, bytes_accessed=4 * cols * width),
    )(dy, out, wo)


def _everyone(row_ref, sum_ref, buf, out_sem, in_sem):
    me = lax.axis_index("tp")
    barrier = pltpu.get_barrier_semaphore()
    others = [lax.rem(me + n, 16) for n in range(1, 16)]
    for other in others:
        pl.semaphore_signal(barrier, inc=1, device_id={"tp": other}, device_id_type=MESH)
    pl.semaphore_wait(barrier, 15)
    copies = [pltpu.make_async_remote_copy(src_ref=row_ref, dst_ref=buf.at[n], send_sem=out_sem.at[n], recv_sem=in_sem.at[n],
                                           device_id={"tp": other}, device_id_type=MESH) for n, other in enumerate(others)]
    for copy in copies:
        copy.start()
    for copy in copies:
        copy.wait_recv()
    total = None
    for i in range(16):
        slot = lax.rem(me - i + 31, 16)
        term = jnp.where(slot == 15, row_ref[...], buf[lax.rem(slot, 15)])
        total = term if total is None else total + term
    sum_ref[...] = total
    for copy in copies:
        copy.wait_send()


def everyone(row):
    shape = (row.shape[1] // 128, 128)
    return pl.pallas_call(
        _everyone,
        in_specs=[WHOLE],
        out_specs=WHOLE,
        out_shape=jax.ShapeDtypeStruct(shape, F32),
        scratch_shapes=[pltpu.VMEM((15, *shape), F32), pltpu.SemaphoreType.DMA((15,)), pltpu.SemaphoreType.DMA((15,))],
        compiler_params=pltpu.CompilerParams(collective_id=4, has_side_effects=True),
        cost_estimate=pl.CostEstimate(flops=2**20, transcendentals=0, bytes_accessed=2**20),
    )(row.reshape(shape)).reshape(row.shape)


def solution(mesh):
    def step(x, dy, gain, wq, wk, wv, wo):
        wide, gain = x.astype(F32), gain.astype(F32)
        scale = lax.rsqrt(jnp.mean(wide * wide, -1, keepdims=True) + 1e-6)
        rows = 16 * x.shape[0]
        half = HEAD // 2
        angle = jnp.arange(rows).astype(F32)[:, None] * THETA ** (-jnp.arange(half, dtype=F32) / half)
        cos, sin = jnp.cos(angle), jnp.sin(angle)
        cos, sin = jnp.concatenate([cos, cos], 1), jnp.concatenate([-sin, sin], 1)

        some, q, k, v = project((wide * scale * gain).astype(BF16), wq, wk, wv)
        out, lse, q, k = attend(q, k, v, cos, sin)
        d_out, by_wo = unproject(dy, out, wo)
        dq, dk, dv = attend_bwd(q, k, v, d_out, out, lse, cos, sin)
        da, by_wq, by_wk, by_wv = tail(dq, dk, dv, wq, wk, wv, some)

        n = wide * scale
        by_gain = everyone((da * n).sum(0, keepdims=True))
        dn = da * gain
        by_x = scale * (dn - n * jnp.mean(dn * n, -1, keepdims=True)) + dy.astype(F32)
        return by_x.astype(BF16), by_gain, by_wq, by_wk, by_wv, by_wo

    tokens, columns = P(("dp", "tp"), None), P(None, "tp")
    return jax.shard_map(
        step,
        mesh=mesh,
        in_specs=(tokens, tokens, P(None), columns, columns, columns, P("tp", None)),
        out_specs=(tokens, P("dp", None), P("dp", "tp"), P("dp", "tp"), P("dp", "tp"), P(("dp", "tp"), None)),
        check_vma=False,
    )
```
